32 devices in a mesh: members: 2 (over y), patch: 4 (over z), feat: 4 (over x, core).
Axes of the slice: x: 2, y: 2, z: 4, core: 2. Of those that a mesh axis runs over, the one named last changes fastest.
Arguments:
- latents: bfloat16 [24576, 512], P(('members', 'patch', 'feat')), parts along dimension 0, may hold values from -6 to 6
- neighbours: int32 [12288, 8], P(('patch', 'feat')), may hold values from 0 to 799
- degree: int32 [12288], P(('patch', 'feat')), may hold values from 4 to 8
- send_rows: int32 [64, 8], P(('patch', 'feat')), may hold values from 0 to 767
- area: float32 [12288], P(('patch', 'feat')), may hold values from 0.3 to 10
- scenario: int32 [6], P('members'), parts along dimension 0, may hold values from 0 to 15
- totals: float32 [16, 3], replicated, may hold values from 0.3 to 1.5
- w_send: bfloat16 [1, 512, 512], P(None, None, 'feat'), may hold values from -0.25 to 0.25
- w_recv: bfloat16 [1, 512, 512], P(None, None, 'feat'), may hold values from -0.25 to 0.25
- b_edge: float32 [1, 512], replicated, may hold values from -3 to 3
- w_msg: bfloat16 [1, 512, 512], P(None, None, 'feat'), may hold values from -0.25 to 0.25
- w_node: bfloat16 [1, 1024, 512], P(None, None, 'feat'), may hold values from -0.1875 to 0.1875
- w_out: bfloat16 [1, 512, 512], P(None, None, 'feat'), may hold values from -0.25 to 0.25
- gain: float32 [1, 512], replicated, may hold values from 0.5 to 1.5
- w_dec: bfloat16 [3, 512], replicated, may hold values from -0.25 to 0.25
- w_enc: float32 [3, 512], replicated, may hold values from -3 to 3
Outputs:
- final_latents: bfloat16 [24576, 512], P(('members', 'patch', 'feat')), parts along dimension 0
- conserved: float32 [4, 3, 12288], P('members', None, ('patch', 'feat')), parts along dimension 0
The draws below stay inside these ranges and needn't reach their ends.
There are 2 independent parts, one for each index of `members`. The reference program is written for one: setup_inputs(seed, part) draws one part's arguments, and reference() takes and returns one part's arrays. A program takes and returns all parts, laid end to end along the dimension named above; an argument that names none is the same for every part. Nothing has to cross between parts.
Inputs may be any that keep to these rules, and one draw needn't show every extreme that they name: `neighbours`: an entry below 768 is a row of the node's own device; entry 768 + j * 8 + t names the t-th row that the device of patch j with the same feat index sends to the node's patch. A node's live slots are its first degree[n] slots. `send_rows`: row q * 4 + i lists rows of device q, in its own numbering, that patch i receives.
All inputs are finite; a program needn't handle non-finite values.
Results may differ from the reference program's by a relative error of at most 0.012.
Values may be sent and summed in bfloat16 or wider, within the bound.
A program may use at most 64 MiB of HBM per device.

```python
import math
import jax
import jax.numpy as jnp
from jax import lax

D = 512
NODE_DEV = 768
DEG = 8
SLOT = 8
LAYERS = 1
STEPS = 2
FIELDS = 3
SCEN = 16
NODES = 12288
N_PATCH = 4
N_FEAT = 4


def draw_area(key, part):
    position = jnp.arange(NODES, dtype=jnp.float32) / NODES
    baseline = 1.0 + 2.0 * position
    level_key = jax.random.fold_in(key, 7)
    level = jnp.exp(jax.random.uniform(level_key, (), jnp.float32, -0.5, 0.5))
    rough = jnp.exp(jax.random.uniform(key, (NODES,), jnp.float32, -0.69, 0.69))
    return (level * baseline * rough).astype(jnp.float32)


def plant(array, own_key, least, high):
    longest = array.shape.index(max(array.shape))
    spots = []
    for shift in (0, 1):
        where = [jax.random.randint(jax.random.fold_in(own_key, axis), (), 0, length) for axis, length in enumerate(array.shape)]
        where[longest] = (where[longest] + shift) % array.shape[longest]
        spots.append(tuple(where))
    return array.at[spots[0]].set(least).at[spots[1]].set(high)


def block_levels(own_key, shape, shards, least, high):
    loudness, own = 1.0, jax.random.fold_in(own_key, 6)
    for axis_at, shards_of in shards:
        draws = jnp.exp(jax.random.uniform(jax.random.fold_in(own, axis_at), (shards_of,), jnp.float32, least / len(shards), high / len(shards)))
        loudness = loudness * jnp.repeat(draws, shape[axis_at] // shards_of).reshape([-1 if axis == axis_at else 1 for axis in range(len(shape))])
    return loudness


def scatter_about(stream_key, shape, width, reach, cuts=(), held_as=jnp.bfloat16):
    result = jax.random.normal(stream_key, shape, jnp.float32) * width
    if len(cuts) > 0:
        result = block_levels(stream_key, shape, cuts, -0.22, 0.18) * result
    return jnp.clip(result, min=-reach, max=reach).astype(held_as)


def setup_inputs(seed: int = 0, part: int = 0) -> dict:
    keys = jax.random.split(jax.random.key(seed), 17)
    part_splits = jax.random.split(jax.random.fold_in(keys[16], part), 17)
    return {
        "latents": scatter_about(part_splits[0], (NODES, D), 1.0, 6.0, ((0, 16),)),
        "neighbours": plant(jax.random.randint(keys[1], (NODES, DEG), 0, NODE_DEV + N_PATCH * SLOT), jax.random.fold_in(keys[1], 1), 0, (NODE_DEV + N_PATCH * SLOT) - 1).astype(jnp.int32),
        "degree": plant(jax.random.randint(keys[2], (NODES,), 4, DEG + 1), jax.random.fold_in(keys[2], 1), 4, DEG).astype(jnp.int32),
        "send_rows": plant(jax.random.randint(keys[3], (N_PATCH * N_FEAT * N_PATCH, SLOT), 0, NODE_DEV), jax.random.fold_in(keys[3], 1), 0, NODE_DEV - 1).astype(jnp.int32),
        "area": draw_area(jax.random.fold_in(keys[16], 71), part),
        "scenario": jax.random.randint(part_splits[5], (FIELDS,), 0, SCEN).astype(jnp.int32),
        "totals": jnp.clip(jnp.exp(jax.random.uniform(keys[6], (SCEN, FIELDS), jnp.float32, math.log(0.3), math.log(1.5))), 0.3, 1.5),
        "w_send": scatter_about(keys[7], (LAYERS, D, D), D ** -0.5, 0.25, ((2, 4),)),
        "w_recv": scatter_about(keys[8], (LAYERS, D, D), D ** -0.5, 0.25, ((2, 4),)),
        "b_edge": scatter_about(keys[9], (LAYERS, D), 0.5, 3.0, (), jnp.float32),
        "w_msg": scatter_about(keys[10], (LAYERS, D, D), D ** -0.5, 0.25, ((2, 4),)),
        "w_node": scatter_about(keys[11], (LAYERS, 2 * D, D), (2 * D) ** -0.5, 0.1875, ((2, 4),)),
        "w_out": scatter_about(keys[12], (LAYERS, D, D), D ** -0.5, 0.25, ((2, 4),)),
        "gain": jnp.clip(1.0 + 0.1 * jax.random.normal(keys[13], (LAYERS, D), jnp.float32), 0.5, 1.5),
        "w_dec": scatter_about(keys[14], (FIELDS, D), D ** -0.5, 0.25),
        "w_enc": scatter_about(keys[15], (FIELDS, D), 0.5, 3.0, (), jnp.float32),
    }


EPSILON = 1e-05

def sender_ids(neighbours, send_rows):
    device = (jnp.arange(NODES, dtype=jnp.int32) // NODE_DEV)[:, None]
    node_patch = device // N_FEAT
    node_feat = device % N_FEAT
    is_local = neighbours < NODE_DEV
    remote = jnp.maximum(neighbours - NODE_DEV, 0)
    source = (remote // SLOT).astype(jnp.int32)
    within = (remote % SLOT).astype(jnp.int32)
    source_dev = source * N_FEAT + node_feat
    sent_row = send_rows[source_dev * N_PATCH + node_patch, within]
    return jnp.where(is_local, device * NODE_DEV + neighbours, source_dev * NODE_DEV + sent_row).astype(jnp.int32)

def layer_update(latent, senders, live_slots, weight_send, weight_recv, bias_edge, weight_msg, weight_node, weight_out, gain_row):
    sender = jnp.dot(latent, weight_send, preferred_element_type=jnp.float32).astype(jnp.bfloat16)
    receiver = jnp.dot(latent, weight_recv, preferred_element_type=jnp.float32) + bias_edge
    summed = jnp.zeros((NODES, D), jnp.float32)
    for position in range(DEG):
        edge_value = sender[senders[:, position]].astype(jnp.float32) + receiver
        summed = summed + jnp.where(live_slots[:, position:position + 1], jax.nn.silu(edge_value), 0.0)
    summed = summed.astype(jnp.bfloat16)
    message = jnp.dot(summed, weight_msg, preferred_element_type=jnp.float32).astype(jnp.bfloat16)
    hidden = jax.nn.silu(jnp.dot(latent, weight_node[:D], preferred_element_type=jnp.float32) + jnp.dot(message, weight_node[D:], preferred_element_type=jnp.float32)).astype(jnp.bfloat16)
    output = jnp.dot(hidden, weight_out, preferred_element_type=jnp.float32)
    average = lax.optimization_barrier(jnp.mean(output, axis=1, keepdims=True))
    variance = lax.optimization_barrier(jnp.mean(jnp.square(output - average), axis=1, keepdims=True))
    normed = (output - average) * lax.rsqrt(variance + EPSILON) * gain_row
    return (latent.astype(jnp.float32) + normed).astype(jnp.bfloat16)

def reference(latents, neighbours, degree, send_rows, area, scenario, totals, w_send, w_recv, b_edge, w_msg, w_node, w_out, gain, w_dec, w_enc):
    senders = sender_ids(neighbours, send_rows)
    live_slots = jnp.arange(DEG, dtype=jnp.int32)[None, :] < degree[:, None]
    chosen = (jnp.arange(SCEN, dtype=jnp.int32)[:, None] == scenario[None, :]).astype(jnp.float32)
    target = lax.optimization_barrier(jnp.sum(chosen * totals, axis=0))
    latent_state = latents
    history = []
    for step_index in range(STEPS):
        for layer_index in range(LAYERS):
            latent_state = layer_update(latent_state, senders, live_slots, w_send[layer_index], w_recv[layer_index], b_edge[layer_index], w_msg[layer_index], w_node[layer_index], w_out[layer_index], gain[layer_index])
        decoded = lax.dot_general(w_dec, latent_state, (((1,), (1,)), ((), ())), preferred_element_type=jnp.float32)
        fields = jax.nn.softplus(decoded)
        integral = lax.optimization_barrier(jnp.sum(area[None, :] * fields, axis=1))
        scale = target * float(NODES) / integral
        history.append(scale[:, None] * fields)
        change = (scale - 1.0)[:, None] * fields
        update = lax.dot_general(change, w_enc, (((0,), (0,)), ((), ())), precision=lax.Precision.HIGHEST, preferred_element_type=jnp.float32)
        latent_state = (latent_state.astype(jnp.float32) + update).astype(jnp.bfloat16)
    return (latent_state, jnp.stack(history))
```

```python
import functools

import jax
import jax.numpy as jnp
from jax import lax
from jax.experimental import pallas as pl
from jax.experimental.pallas import tpu as pltpu
from jax.sharding import PartitionSpec as P

STEPS = 2
EPSILON = 1e-05
DEAD = -1e30
MESH = pl.DeviceIdType.MESH
ROWS = 128


def dot(a, b):
    return jnp.dot(a, b, preferred_element_type=jnp.float32)


def kernel(
    n_patch,
    n_feat,
    lat_ref,
    nb_ref,
    deg_ref,
    send_ref,
    area_ref,
    scen_ref,
    tot_ref,
    ws_ref,
    wr_ref,
    be_ref,
    wm_ref,
    wn_ref,
    wo_ref,
    gain_ref,
    wdec_ref,
    wenc_ref,
    out_ref,
    cons_ref,
    ws,
    wr,
    wm,
    wn,
    wo,
    onehot,
    table,
    gathered,
    hext,
    receiver,
    esum,
    wdec,
    halo_out,
    halo_in,
    part_out,
    part_in,
    w_send_sem,
    w_recv_sem,
    halo_send_sem,
    halo_recv_sem,
    part_send_sem,
    part_recv_sem,
):
    n, width = lat_ref.shape
    slots = nb_ref.shape[1]
    slot_rows = send_ref.shape[1]
    n_fields = wdec_ref.shape[0]
    halo_rows = n_patch * slot_rows
    ext = n + halo_rows
    padded = table.shape[0]
    group = n_patch * n_feat
    chunks = n // ROWS
    patch = lax.axis_index("patch")
    feat = lax.axis_index("feat")
    me = patch * n_feat + feat
    node_count = float(n * group)

    def peer(d):
        other = lax.rem(me + d, group)
        return {"patch": other // n_feat, "feat": lax.rem(other, n_feat)}

    barrier = pltpu.get_barrier_semaphore()

    @pl.loop(1, group)
    def _(d):
        pl.semaphore_signal(barrier, inc=1, device_id=peer(d), device_id_type=MESH)

    def halo_pick(rows):
        pieces = []
        node = lax.broadcasted_iota(jnp.int32, (slot_rows, n), 1)
        picked = send_t
        hot = jnp.where(lax.broadcasted_iota(jnp.int32, (halo_rows, n), 1) == picked, 1.0, 0.0)
        return dot(hot.astype(jnp.bfloat16), rows)

    row_at = lax.broadcasted_iota(jnp.int32, (halo_rows, slot_rows), 0)
    lane_at = lax.broadcasted_iota(jnp.int32, (halo_rows, slot_rows), 1)
    spread = jnp.concatenate(
        [jnp.broadcast_to(send_ref[q : q + 1, :], (slot_rows, slot_rows)) for q in range(n_patch)],
        axis=0,
    )
    send_t = jnp.sum(
        jnp.where(lax.rem(row_at, slot_rows) == lane_at, spread.astype(jnp.float32), 0.0),
        axis=1,
        keepdims=True,
    ).astype(jnp.int32)

    halo_out[0] = halo_pick(lat_ref[...])

    pl.semaphore_wait(barrier, group - 1)

    pairs = n_feat // 2
    pair, core = feat // 2, lax.rem(feat, 2)
    partner = pair * 2 + 1 - core
    sources = (ws_ref, wr_ref, wm_ref, wn_ref, wo_ref)
    wholes = (ws, wr, wm, wn, wo)
    piece = ws_ref.shape[2]

    def columns(owner):
        return pl.ds(pl.multiple_of(owner * piece, piece), piece)

    across, beside, relays = [], [], []
    for w, (source, whole) in enumerate(zip(sources, wholes)):
        for d in range(1, pairs):
            copy = pltpu.make_async_remote_copy(
                src_ref=source.at[0],
                dst_ref=whole.at[:, columns(feat)],
                send_sem=w_send_sem.at[w, d],
                recv_sem=w_recv_sem.at[w, d],
                device_id={"feat": lax.rem(pair + d, pairs) * 2 + core},
                device_id_type=MESH,
            )
            copy.start()
            across.append(copy)
    for w, (source, whole) in enumerate(zip(sources, wholes)):
        copy = pltpu.make_async_remote_copy(
            src_ref=source.at[0],
            dst_ref=whole.at[:, columns(feat)],
            send_sem=w_send_sem.at[w, 0],
            recv_sem=w_recv_sem.at[w, 0],
            device_id={"feat": partner},
            device_id_type=MESH,
        )
        copy.start()
        beside.append(copy)

    def halo_copy(step, d):
        other = lax.rem(patch + d, n_patch)
        return pltpu.make_async_remote_copy(
            src_ref=halo_out.at[step, pl.ds(pl.multiple_of(other * slot_rows, slot_rows), slot_rows)],
            dst_ref=halo_in.at[step, pl.ds(pl.multiple_of(patch * slot_rows, slot_rows), slot_rows)],
            send_sem=halo_send_sem.at[step],
            recv_sem=halo_recv_sem.at[step],
            device_id={"patch": other},
            device_id_type=MESH,
        )

    def halo_start(step):
        @pl.loop(1, n_patch)
        def _(d):
            halo_copy(step, d).start()

        own = pl.ds(pl.multiple_of(patch * slot_rows, slot_rows), slot_rows)
        halo_in[step, own, :] = halo_out[step, own, :]

    def halo_all(step, sem):
        many = pl.ds(0, (n_patch - 1) * slot_rows)
        return pltpu.make_async_copy(halo_out.at[step, many], halo_in.at[step, many], sem)

    def part_copy(step, d):
        return pltpu.make_async_remote_copy(
            src_ref=part_out.at[step],
            dst_ref=part_in.at[step, me],
            send_sem=part_send_sem.at[step],
            recv_sem=part_recv_sem.at[step],
            device_id=peer(d),
            device_id_type=MESH,
        )

    def part_all(step, sem):
        many = pl.ds(0, group - 1)
        return pltpu.make_async_copy(part_in.at[step, many], part_in.at[step, many], sem)

    halo_start(0)
    for source, whole in zip(sources, wholes):
        whole[:, columns(feat)] = source[0]

    wdec[...] = jnp.zeros_like(wdec)
    wdec[0:n_fields, :] = wdec_ref[...].astype(jnp.float32)
    table[ext:, :] = jnp.full((padded - ext, width), DEAD, table.dtype)

    @pl.loop(0, chunks)
    def _(c):
        rows = pl.ds(pl.multiple_of(c * ROWS, ROWS), ROWS)
        degree = jnp.transpose(jnp.broadcast_to(deg_ref[:, rows], (8, ROWS)))[:, 0:1]
        for k in range(slots):
            target = jnp.where(degree > k, nb_ref[rows, k : k + 1], ext)
            hot = lax.broadcasted_iota(jnp.int32, (ROWS, padded), 1) == target
            onehot[c, k * ROWS : (k + 1) * ROWS, :] = jnp.where(hot, 1.0, 0.0).astype(jnp.bfloat16)

    field_row = lax.broadcasted_iota(jnp.int32, (8, 1), 0)
    target = jnp.zeros((8, 1), jnp.float32)
    for f in range(n_fields):
        target = jnp.where(field_row == f, tot_ref[scen_ref[f], f], target)

    hext[0:n, :] = lat_ref[...]
    halo_all(0, halo_recv_sem.at[0]).wait()
    hext[n:, :] = halo_in[0].astype(jnp.bfloat16)

    def relay(w):
        whole = wholes[w]
        for d in range(1, pairs):
            across[w * (pairs - 1) + d - 1].wait_recv()
            block = whole.at[:, columns(lax.rem(pair + pairs - d, pairs) * 2 + core)]
            copy = pltpu.make_async_remote_copy(
                src_ref=block,
                dst_ref=block,
                send_sem=w_send_sem.at[w, pairs + d - 1],
                recv_sem=w_recv_sem.at[w, pairs + d - 1],
                device_id={"feat": partner},
                device_id_type=MESH,
            )
            copy.start()
            relays.append(copy)

    def arrived(w):
        beside[w].wait_recv()
        for d in range(1, pairs):
            relays[w * (pairs - 1) + d - 1].wait_recv()

    for step in range(STEPS):
        if step == 0:
            relay(0)
            relay(1)
            arrived(0)
        table[0:ext, :] = (0.5 * dot(hext[...], ws[...]).astype(jnp.bfloat16)).astype(jnp.bfloat16)
        if step == 0:
            arrived(1)
        receiver[...] = 0.5 * (dot(hext[0:n, :], wr[...]) + be_ref[0:1, :])

        @pl.loop(0, chunks)
        def _(c):
            rows = pl.ds(pl.multiple_of(c * ROWS, ROWS), ROWS)
            gathered[...] = dot(onehot[c], table[...])
            base = receiver[rows, :]
            total = jnp.zeros((ROWS, width), jnp.float32)
            for k in range(slots):
                half = gathered[k * ROWS : (k + 1) * ROWS, :] + base
                total = total + (half + half * jnp.tanh(half))
            esum[rows, :] = total.astype(jnp.bfloat16)

        if step == 0:
            for w in (2, 3, 4):
                relay(w)
            for w in (2, 3, 4):
                arrived(w)

        @pl.loop(0, chunks // 2)
        def _(c):
            rows = pl.ds(pl.multiple_of(c * 2 * ROWS, 2 * ROWS), 2 * ROWS)
            latent = hext[rows, :]
            message = dot(esum[rows, :], wm[...]).astype(jnp.bfloat16)
            half = 0.5 * (dot(latent, wn[0:width, :]) + dot(message, wn[width:, :]))
            hidden = (half + half * jnp.tanh(half)).astype(jnp.bfloat16)
            output = dot(hidden, wo[...])
            average = jnp.mean(output, axis=1, keepdims=True)
            centred = output - average
            variance = jnp.mean(jnp.square(centred), axis=1, keepdims=True)
            normed = centred * lax.rsqrt(variance + EPSILON) * gain_ref[0:1, :]
            hext[rows, :] = (latent.astype(jnp.float32) + normed).astype(jnp.bfloat16)

        def decode(rows):
            raw = lax.dot_general(
                wdec[...].astype(jnp.bfloat16),
                rows,
                (((1,), (1,)), ((), ())),
                preferred_element_type=jnp.float32,
            )
            return jnp.maximum(raw, 0.0) + jnp.log1p(jnp.exp(-jnp.abs(raw)))

        fields = decode(hext[0:n, :])
        part = jnp.sum(area_ref[...] * fields, axis=1, keepdims=True)
        part = jnp.broadcast_to(part, part_out.shape[1:])
        part_out[step] = part
        part_in[step, me] = part

        @pl.loop(1, group)
        def _(d):
            part_copy(step, d).start()

        last = step == STEPS - 1
        count = n if last else ext
        if not last:
            halo_out[step + 1] = halo_pick(hext[0:n, :])
            halo_start(step + 1)
        fields_t = [jnp.transpose(fields)]
        if not last:
            halo_all(step + 1, halo_recv_sem.at[step + 1]).wait()
            arrived_rows = halo_in[step + 1].astype(jnp.bfloat16)
            hext[n:, :] = arrived_rows
            raw = lax.dot_general(
                arrived_rows,
                wdec[...].astype(jnp.bfloat16),
                (((1,), (1,)), ((), ())),
                preferred_element_type=jnp.float32,
            )
            fields_t.append(jnp.maximum(raw, 0.0) + jnp.log1p(jnp.exp(-jnp.abs(raw))))

        part_all(step, part_recv_sem.at[step]).wait()
        integral = jnp.sum(part_in[step], axis=0)[:, 0:1]
        scale = target * node_count / integral
        cons_ref[step] = (scale * fields)[0:n_fields, :]
        change = (scale - 1.0)[0:n_fields] * wenc_ref[...]
        start = 0
        for block in fields_t:
            size = block.shape[0]
            update = block[:, 0:1] * change[0:1, :]
            for f in range(1, n_fields):
                update = update + block[:, f : f + 1] * change[f : f + 1, :]
            moved = (hext[start : start + size, :].astype(jnp.float32) + update).astype(jnp.bfloat16)
            if last:
                out_ref[...] = moved
            else:
                hext[start : start + size, :] = moved
            start += size

    for copy in across + beside + relays:
        copy.wait_send()
    for step in range(STEPS):
        halo_all(step, halo_send_sem.at[step]).wait()
        part_all(step, part_send_sem.at[step]).wait()


def solution(mesh):
    n_patch, n_feat = mesh.shape["patch"], mesh.shape["feat"]

    def shards(
        latents,
        neighbours,
        degree,
        send_rows,
        area,
        scenario,
        totals,
        w_send,
        w_recv,
        b_edge,
        w_msg,
        w_node,
        w_out,
        gain,
        w_dec,
        w_enc,
    ):
        n, width = latents.shape
        slots = neighbours.shape[1]
        halo_rows = n_patch * send_rows.shape[1]
        ext = n + halo_rows
        padded = (ext + 256) // 256 * 256
        group = n_patch * n_feat
        n_fields = w_dec.shape[0]
        vmem = pl.BlockSpec(memory_space=pltpu.VMEM)
        smem = pl.BlockSpec(memory_space=pltpu.SMEM)
        bf16, f32 = jnp.bfloat16, jnp.float32
        return pl.pallas_call(
            functools.partial(kernel, n_patch, n_feat),
            out_shape=(
                jax.ShapeDtypeStruct((n, width), bf16),
                jax.ShapeDtypeStruct((STEPS, n_fields, n), f32),
            ),
            in_specs=[vmem] * 5 + [smem] * 2 + [vmem] * 9,
            out_specs=(vmem, vmem),
            scratch_shapes=[
                pltpu.VMEM((width, width), bf16),
                pltpu.VMEM((width, width), bf16),
                pltpu.VMEM((width, width), bf16),
                pltpu.VMEM((2 * width, width), bf16),
                pltpu.VMEM((width, width), bf16),
                pltpu.VMEM((n // ROWS, slots * ROWS, padded), bf16),
                pltpu.VMEM((padded, width), bf16),
                pltpu.VMEM((slots * ROWS, width), f32),
                pltpu.VMEM((ext, width), bf16),
                pltpu.VMEM((n, width), f32),
                pltpu.VMEM((n, width), bf16),
                pltpu.VMEM((8, width), f32),
                pltpu.VMEM((STEPS, halo_rows, width), f32),
                pltpu.VMEM((STEPS, halo_rows, width), f32),
                pltpu.VMEM((STEPS, 8, 128), f32),
                pltpu.VMEM((STEPS, group, 8, 128), f32),
                pltpu.SemaphoreType.DMA((5, n_feat)),
                pltpu.SemaphoreType.DMA((5, n_feat)),
                pltpu.SemaphoreType.DMA((STEPS,)),
                pltpu.SemaphoreType.DMA((STEPS,)),
                pltpu.SemaphoreType.DMA((STEPS,)),
                pltpu.SemaphoreType.DMA((STEPS,)),
            ],
            compiler_params=pltpu.CompilerParams(
                collective_id=0, has_side_effects=True, vmem_limit_bytes=60 * 1024 * 1024
            ),
        )(
            latents,
            neighbours,
            degree.reshape(1, n),
            send_rows,
            area.reshape(1, n),
            scenario,
            totals,
            w_send,
            w_recv,
            b_edge,
            w_msg,
            w_node,
            w_out,
            gain,
            w_dec,
            w_enc,
        )

    in_specs = (
        P(("members", "patch", "feat"), None),
        P(("patch", "feat"), None),
        P(("patch", "feat")),
        P(("patch", "feat"), None),
        P(("patch", "feat")),
        P("members"),
        P(),
        P(None, None, "feat"),
        P(None, None, "feat"),
        P(),
        P(None, None, "feat"),
        P(None, None, "feat"),
        P(None, None, "feat"),
        P(),
        P(),
        P(),
    )
    out_specs = (P(("members", "patch", "feat"), None), P("members", None, ("patch", "feat")))
    return jax.shard_map(shards, mesh=mesh, in_specs=in_specs, out_specs=out_specs, check_vma=False)
```

```python
import functools

import jax
import jax.numpy as jnp
from jax import lax
from jax.experimental import pallas as pl
from jax.experimental.pallas import tpu as pltpu
from jax.sharding import PartitionSpec as P

STEPS = 2
EPSILON = 1e-05
DEAD = -1e30
INPUTS = 16
VMEM_BYTES = 67043328
MESH = pl.DeviceIdType.MESH
ROWS = 128


def dot(a, b):
    return jnp.dot(a, b, preferred_element_type=jnp.float32)


def rescaled(latent, fields_t, change):
    update = fields_t[:, 0:1] * change[0:1, :]
    for f in range(1, change.shape[0]):
        update = update + fields_t[:, f : f + 1] * change[f : f + 1, :]
    return (latent.astype(jnp.float32) + update).astype(jnp.bfloat16)


def finish(lat_ref, fields_ref, scale_ref, change_ref, out_ref, cons_ref):
    n_fields = change_ref.shape[0]
    for step in range(STEPS):
        kept = scale_ref[step][:, 0:1] * fields_ref[step]
        for f in range(n_fields):
            cons_ref[f, step : step + 1, :] = kept[f : f + 1, :]
    fields_t = jnp.transpose(fields_ref[STEPS - 1])
    out_ref[...] = rescaled(lat_ref[...], fields_t, change_ref[...])


def kernel(
    n_patch,
    n_feat,
    *refs,
):
    held, (out_ref, fields_ref, scale_ref, change_ref) = refs[:INPUTS], refs[INPUTS : INPUTS + 4]
    loaded = refs[INPUTS + 4 : 2 * INPUTS + 4]
    (
        lat_ref,
        nb_ref,
        deg_ref,
        send_ref,
        area_ref,
        scen_ref,
        tot_ref,
        ws_ref,
        wr_ref,
        be_ref,
        wm_ref,
        wn_ref,
        wo_ref,
        gain_ref,
        wdec_ref,
        wenc_ref,
    ) = loaded
    (
        load_sem,
        ws,
        wr,
        wm,
        wn,
        wo,
        onehot,
        table,
        gathered_a,
        gathered_b,
        hext,
        receiver,
        esum,
        wdec,
        halo_out,
        halo_in,
        part_out,
        part_in,
        w_send_sem,
        w_recv_sem,
        halo_send_sem,
        halo_recv_sem,
        part_send_sem,
        part_recv_sem,
    ) = refs[2 * INPUTS + 4 :]
    loads = [
        pltpu.make_async_copy(source, here, load_sem.at[i])
        for i, (source, here) in enumerate(zip(held, loaded))
    ]
    for load in loads:
        load.start()
    n, width = lat_ref.shape
    slots = nb_ref.shape[0]
    slot_rows = send_ref.shape[1]
    n_fields = wdec_ref.shape[0]
    halo_rows = n_patch * slot_rows
    ext = n + halo_rows
    padded = table.shape[0]
    group = n_patch * n_feat
    chunks = n // ROWS
    patch = lax.axis_index("patch")
    feat = lax.axis_index("feat")
    me = patch * n_feat + feat
    node_count = float(n * group)

    def peer(d):
        other = lax.rem(me + d, group)
        return {"patch": other // n_feat, "feat": lax.rem(other, n_feat)}

    barrier = pltpu.get_barrier_semaphore()

    @pl.loop(1, group)
    def _(d):
        pl.semaphore_signal(barrier, inc=1, device_id=peer(d), device_id_type=MESH)

    for load in loads:
        load.wait()

    def halo_pick(rows):
        node = lax.broadcasted_iota(jnp.int32, (halo_rows, n), 1)
        hot = jnp.where(node == send_t, 1.0, 0.0)
        return dot(hot.astype(jnp.bfloat16), rows)

    row_at = lax.broadcasted_iota(jnp.int32, (halo_rows, slot_rows), 0)
    lane_at = lax.broadcasted_iota(jnp.int32, (halo_rows, slot_rows), 1)
    spread = jnp.concatenate(
        [jnp.broadcast_to(send_ref[q : q + 1, :], (slot_rows, slot_rows)) for q in range(n_patch)],
        axis=0,
    )
    send_t = jnp.sum(
        jnp.where(lax.rem(row_at, slot_rows) == lane_at, spread.astype(jnp.float32), 0.0),
        axis=1,
        keepdims=True,
    ).astype(jnp.int32)

    halo_out[0] = halo_pick(lat_ref[...])

    pl.semaphore_wait(barrier, group - 1)

    pairs = n_feat // 2
    pair, core = feat // 2, lax.rem(feat, 2)
    partner = pair * 2 + 1 - core
    sources = (ws_ref, wr_ref, wm_ref, wn_ref, wo_ref)
    wholes = (ws, wr, wm, wn, wo)
    piece = ws_ref.shape[2]

    def columns(owner):
        return pl.ds(pl.multiple_of(owner * piece, piece), piece)

    across, beside, relays = [], [], []
    for w, (source, whole) in enumerate(zip(sources, wholes)):
        for d in range(1, pairs):
            copy = pltpu.make_async_remote_copy(
                src_ref=source.at[0],
                dst_ref=whole.at[:, columns(feat)],
                send_sem=w_send_sem.at[w, d],
                recv_sem=w_recv_sem.at[w, d],
                device_id={"feat": lax.rem(pair + d, pairs) * 2 + core},
                device_id_type=MESH,
            )
            copy.start()
            across.append(copy)
    for w, (source, whole) in enumerate(zip(sources, wholes)):
        copy = pltpu.make_async_remote_copy(
            src_ref=source.at[0],
            dst_ref=whole.at[:, columns(feat)],
            send_sem=w_send_sem.at[w, 0],
            recv_sem=w_recv_sem.at[w, 0],
            device_id={"feat": partner},
            device_id_type=MESH,
        )
        copy.start()
        beside.append(copy)

    def halo_copy(step, d):
        other = lax.rem(patch + d, n_patch)
        return pltpu.make_async_remote_copy(
            src_ref=halo_out.at[step, pl.ds(pl.multiple_of(other * slot_rows, slot_rows), slot_rows)],
            dst_ref=halo_in.at[step, pl.ds(pl.multiple_of(patch * slot_rows, slot_rows), slot_rows)],
            send_sem=halo_send_sem.at[step],
            recv_sem=halo_recv_sem.at[step],
            device_id={"patch": other},
            device_id_type=MESH,
        )

    def halo_start(step):
        @pl.loop(1, n_patch)
        def _(d):
            halo_copy(step, d).start()

        own = pl.ds(pl.multiple_of(patch * slot_rows, slot_rows), slot_rows)
        halo_in[step, own, :] = halo_out[step, own, :]

    def halo_all(step, sem):
        many = pl.ds(0, (n_patch - 1) * slot_rows)
        return pltpu.make_async_copy(halo_out.at[step, many], halo_in.at[step, many], sem)

    def part_copy(step, d):
        return pltpu.make_async_remote_copy(
            src_ref=part_out.at[step],
            dst_ref=part_in.at[step, me],
            send_sem=part_send_sem.at[step],
            recv_sem=part_recv_sem.at[step],
            device_id=peer(d),
            device_id_type=MESH,
        )

    def part_all(step, sem):
        many = pl.ds(0, group - 1)
        return pltpu.make_async_copy(part_in.at[step, many], part_in.at[step, many], sem)

    halo_start(0)
    for source, whole in zip(sources, wholes):
        whole[:, columns(feat)] = source[0]

    wdec[...] = jnp.zeros_like(wdec)
    wdec[0:n_fields, :] = wdec_ref[...].astype(jnp.float32)
    table[ext:, :] = jnp.full((padded - ext, width), DEAD, table.dtype)

    @pl.loop(0, chunks)
    def _(c):
        rows = pl.ds(pl.multiple_of(c * ROWS, ROWS), ROWS)
        degree = jnp.broadcast_to(deg_ref[rows].reshape(1, ROWS), (slots, ROWS))
        slot_at = lax.broadcasted_iota(jnp.int32, (slots, ROWS), 0)
        wanted = jnp.transpose(jnp.where(slot_at < degree, nb_ref[:, rows], ext))
        for k in range(slots):
            hot = lax.broadcasted_iota(jnp.int32, (ROWS, padded), 1) == wanted[:, k : k + 1]
            onehot[c, k * ROWS : (k + 1) * ROWS, :] = jnp.where(hot, 1.0, 0.0).astype(jnp.bfloat16)

    field_row = lax.broadcasted_iota(jnp.int32, (8, 1), 0)
    target = jnp.zeros((8, 1), jnp.float32)
    for f in range(n_fields):
        target = jnp.where(field_row == f, tot_ref[f, scen_ref[f]], target)

    hext[0:n, :] = lat_ref[...]
    halo_all(0, halo_recv_sem.at[0]).wait()
    hext[n:, :] = halo_in[0].astype(jnp.bfloat16)

    def relay(w):
        whole = wholes[w]
        for d in range(1, pairs):
            across[w * (pairs - 1) + d - 1].wait_recv()
            block = whole.at[:, columns(lax.rem(pair + pairs - d, pairs) * 2 + core)]
            copy = pltpu.make_async_remote_copy(
                src_ref=block,
                dst_ref=block,
                send_sem=w_send_sem.at[w, pairs + d - 1],
                recv_sem=w_recv_sem.at[w, pairs + d - 1],
                device_id={"feat": partner},
                device_id_type=MESH,
            )
            copy.start()
            relays.append(copy)

    def arrived(w):
        beside[w].wait_recv()
        for d in range(1, pairs):
            relays[w * (pairs - 1) + d - 1].wait_recv()

    for step in range(STEPS):
        if step == 0:
            relay(0)
            relay(1)
            arrived(0)
        table[0:ext, :] = (0.5 * dot(hext[...], ws[...]).astype(jnp.bfloat16)).astype(jnp.bfloat16)
        if step == 0:
            arrived(1)
        receiver[...] = 0.5 * (dot(hext[0:n, :], wr[...]) + be_ref[0:1, :])

        def fetch(c, held):
            held[...] = dot(onehot[c], table[...])

        def edges(c, held):
            rows = pl.ds(pl.multiple_of(c * ROWS, ROWS), ROWS)
            base = receiver[rows, :]
            total = jnp.zeros((ROWS, width), jnp.float32)
            for k in range(slots):
                half = held[k * ROWS : (k + 1) * ROWS, :] + base
                total = total + (half + half * jnp.tanh(half))
            esum[rows, :] = total.astype(jnp.bfloat16)

        fetch(0, gathered_a)

        @pl.loop(0, chunks // 2 - 1)
        def _(i):
            fetch(2 * i + 1, gathered_b)
            edges(2 * i, gathered_a)
            fetch(2 * i + 2, gathered_a)
            edges(2 * i + 1, gathered_b)

        if step == 0:
            relay(2)
        fetch(chunks - 1, gathered_b)
        edges(chunks - 2, gathered_a)
        if step == 0:
            relay(3)
        edges(chunks - 1, gathered_b)

        if step == 0:
            relay(4)
            for w in (2, 3, 4):
                arrived(w)

        last = step == STEPS - 1
        latent_next = out_ref if last else hext
        for c in range(chunks // 2):
            rows = slice(c * 2 * ROWS, (c + 1) * 2 * ROWS)
            latent = hext[rows, :]
            message = dot(esum[rows, :], wm[...]).astype(jnp.bfloat16)
            half = 0.5 * (dot(latent, wn[0:width, :]) + dot(message, wn[width:, :]))
            hidden = (half + half * jnp.tanh(half)).astype(jnp.bfloat16)
            output = dot(hidden, wo[...])
            average = jnp.mean(output, axis=1, keepdims=True)
            centred = output - average
            variance = jnp.mean(jnp.square(centred), axis=1, keepdims=True)
            normed = centred * lax.rsqrt(variance + EPSILON) * gain_ref[0:1, :]
            latent_next[rows, :] = (latent.astype(jnp.float32) + normed).astype(jnp.bfloat16)

        def decode(rows):
            raw = lax.dot_general(
                wdec[...].astype(jnp.bfloat16),
                rows,
                (((1,), (1,)), ((), ())),
                preferred_element_type=jnp.float32,
            )
            return jnp.maximum(raw, 0.0) + jnp.log1p(jnp.exp(-jnp.abs(raw)))

        fields = decode(latent_next[0:n, :])
        fields_ref[step] = fields
        part = jnp.sum(area_ref[...].reshape(1, n) * fields, axis=1, keepdims=True)
        part = jnp.broadcast_to(part, part_out.shape[1:])
        part_out[step] = part
        part_in[step, me] = part

        @pl.loop(1, group)
        def _(d):
            part_copy(step, d).start()

        if not last:
            halo_out[step + 1] = halo_pick(hext[0:n, :])
            halo_start(step + 1)
            fields_t = jnp.transpose(fields)
            halo_all(step + 1, halo_recv_sem.at[step + 1]).wait()
            hext[n:, :] = halo_in[step + 1].astype(jnp.bfloat16)
            halo_t = jnp.transpose(decode(hext[n:, :]))

        part_all(step, part_recv_sem.at[step]).wait()
        scale = target * node_count / jnp.sum(part_in[step], axis=0)
        scale_ref[step] = scale
        change = (scale[0:n_fields, 0:1] - 1.0) * wenc_ref[...]
        if last:
            change_ref[...] = change
        else:
            hext[0:n, :] = rescaled(hext[0:n, :], fields_t, change)
            hext[n:, :] = rescaled(hext[n:, :], halo_t, change)

    for copy in across + beside + relays:
        copy.wait_send()
    for step in range(STEPS):
        halo_all(step, halo_send_sem.at[step]).wait()
        part_all(step, part_send_sem.at[step]).wait()


def solution(mesh):
    n_patch, n_feat = mesh.shape["patch"], mesh.shape["feat"]

    def shards(
        latents,
        neighbours,
        degree,
        send_rows,
        area,
        scenario,
        totals,
        w_send,
        w_recv,
        b_edge,
        w_msg,
        w_node,
        w_out,
        gain,
        w_dec,
        w_enc,
    ):
        n, width = latents.shape
        slots = neighbours.shape[1]
        halo_rows = n_patch * send_rows.shape[1]
        ext = n + halo_rows
        padded = (ext + 256) // 256 * 256
        group = n_patch * n_feat
        n_fields = w_dec.shape[0]
        vmem = pl.BlockSpec(memory_space=pltpu.VMEM)
        bf16, f32 = jnp.bfloat16, jnp.float32
        operands = (
            latents,
            neighbours.T,
            degree,
            send_rows,
            area,
            scenario,
            totals.T,
            w_send,
            w_recv,
            b_edge,
            w_msg,
            w_node,
            w_out,
            gain,
            w_dec,
            w_enc,
        )
        places = [pltpu.VMEM] * 5 + [pltpu.SMEM] * 2 + [pltpu.VMEM] * 9
        latent, fields, scale, change = pl.pallas_call(
            functools.partial(kernel, n_patch, n_feat),
            out_shape=(
                jax.ShapeDtypeStruct((n, width), bf16),
                jax.ShapeDtypeStruct((STEPS, 8, n), f32),
                jax.ShapeDtypeStruct((STEPS, 8, 128), f32),
                jax.ShapeDtypeStruct((n_fields, width), f32),
            ),
            in_specs=[pl.BlockSpec(memory_space=pltpu.HBM)] * INPUTS,
            out_specs=(vmem, vmem, vmem, vmem),
            scratch_shapes=[place(x.shape, x.dtype) for place, x in zip(places, operands)]
            + [
                pltpu.SemaphoreType.DMA((INPUTS,)),
                pltpu.VMEM((width, width), bf16),
                pltpu.VMEM((width, width), bf16),
                pltpu.VMEM((width, width), bf16),
                pltpu.VMEM((2 * width, width), bf16),
                pltpu.VMEM((width, width), bf16),
                pltpu.VMEM((n // ROWS, slots * ROWS, padded), bf16),
                pltpu.VMEM((padded, width), bf16),
                pltpu.VMEM((slots * ROWS, width), f32),
                pltpu.VMEM((slots * ROWS, width), f32),
                pltpu.VMEM((ext, width), bf16),
                pltpu.VMEM((n, width), f32),
                pltpu.VMEM((n, width), bf16),
                pltpu.VMEM((8, width), f32),
                pltpu.VMEM((STEPS, halo_rows, width), f32),
                pltpu.VMEM((STEPS, halo_rows, width), f32),
                pltpu.VMEM((STEPS, 8, 128), f32),
                pltpu.VMEM((STEPS, group, 8, 128), f32),
                pltpu.SemaphoreType.DMA((5, n_feat)),
                pltpu.SemaphoreType.DMA((5, n_feat)),
                pltpu.SemaphoreType.DMA((STEPS,)),
                pltpu.SemaphoreType.DMA((STEPS,)),
                pltpu.SemaphoreType.DMA((STEPS,)),
                pltpu.SemaphoreType.DMA((STEPS,)),
            ],
            compiler_params=pltpu.CompilerParams(
                collective_id=0, has_side_effects=True, vmem_limit_bytes=VMEM_BYTES
            ),
        )(
            *operands
        )
        final, conserved = pl.pallas_call(
            finish,
            out_shape=(
                jax.ShapeDtypeStruct((n, width), bf16),
                jax.ShapeDtypeStruct((n_fields, STEPS, n), f32),
            ),
            in_specs=[vmem] * 4,
            out_specs=(vmem, vmem),
            compiler_params=pltpu.CompilerParams(vmem_limit_bytes=VMEM_BYTES),
        )(latent, fields, scale, change)
        return final, conserved.transpose(1, 0, 2)

    in_specs = (
        P(("members", "patch", "feat"), None),
        P(("patch", "feat"), None),
        P(("patch", "feat")),
        P(("patch", "feat"), None),
        P(("patch", "feat")),
        P("members"),
        P(),
        P(None, None, "feat"),
        P(None, None, "feat"),
        P(),
        P(None, None, "feat"),
        P(None, None, "feat"),
        P(None, None, "feat"),
        P(),
        P(),
        P(),
    )
    out_specs = (P(("members", "patch", "feat"), None), P("members", None, ("patch", "feat")))
    return jax.shard_map(shards, mesh=mesh, in_specs=in_specs, out_specs=out_specs, check_vma=False)
```
